32 devices in a mesh: fsdp: 8 (over z, x), rep: 4 (over y, core).
Axes of the slice: x: 2, y: 2, z: 4, core: 2. Of those that a mesh axis runs over, the one named last changes fastest.
Arguments:
- partials: bfloat16 [4, 56, 1024, 1024], P('rep', None, 'fsdp'), may hold values from -400 to 400
- sketch: bfloat16 [8, 4, 2, 1024, 256], P('fsdp', 'rep'), may hold values from -3 to 3
- owner_table: int32 [56, 1], replicated, may hold values from 0 to 7; in each aligned block of 14 rows (0 to 13, 14 to 27, ...) at most 2 rows name the same one
Outputs:
- update: bfloat16 [56, 1024, 1024], P('rep', 'fsdp')
- new_sketch: bfloat16 [8, 4, 2, 1024, 256], P('fsdp', 'rep')
The draws below stay inside these ranges and needn't reach their ends.
Inputs may be any that keep to these rules, and one draw needn't show every extreme that they name: `owner_table`: in each aligned slice of 14 blocks no owner holds more than 2 blocks; some owner holds exactly 2 in some slice.
All inputs are finite; a program needn't handle non-finite values.
Results may differ from the reference program's by a relative error of at most 0.015.
Values may be sent and summed in bfloat16 or wider, within the bound.
A program may use at most 128 MiB of HBM per device.

```python
import math
import jax
import jax.numpy as jnp
import numpy as np
from jax import lax

BS = 1024
RANK = 256
SLOTS = 2
NS_ITERS = 5
BLK_REP = 14
NB = 56
N_FSDP = 8
N_REP = 4


def draw_partials(key, part):
    row_key, column_key, noise_key = jax.random.split(key, 3)
    row_scale = jnp.exp(jax.random.uniform(row_key, (NB, BS, 1), jnp.float32) * math.log(10.0))
    column_scale = jnp.exp(jax.random.uniform(column_key, (NB, 1, BS), jnp.float32) * math.log(10.0))
    block_place = jnp.arange(NB, dtype=jnp.float32) / NB
    row_place = jnp.arange(BS, dtype=jnp.float32) / BS
    trend = jnp.exp(0.5 * math.log(3.0) * (block_place[:, None, None] + row_place[None, :, None]))
    amplitude = 0.1 * row_scale * column_scale * trend

    def replica(number):
        noise = jnp.clip(jax.random.normal(jax.random.fold_in(noise_key, number), (NB, BS, BS), jnp.float32), -6.0, 6.0)
        return (amplitude * noise).astype(jnp.bfloat16)
    return lax.map(replica, jnp.arange(N_REP, dtype=jnp.int32))


def steps_of(stream_key, dims, shards, smallest, top_value):
    level, own = 1.0, jax.random.fold_in(stream_key, 6)
    for axis_at, shards_of in shards:
        steps = jnp.exp(jax.random.uniform(jax.random.fold_in(own, axis_at), (shards_of,), jnp.float32, smallest / len(shards), top_value / len(shards)))
        level = level * jnp.repeat(steps, dims[axis_at] // shards_of).reshape([-1 if axis == axis_at else 1 for axis in range(len(dims))])
    return level


def assign_block(own_key, own, number, rows, number_of, top, bound, slope):
    ranking = jax.random.permutation(own_key, number_of)
    heavy_load, ordinary = load_shares(number_of, rows * top, bound, slope, True), load_shares(number_of, rows * top, bound, slope, False)
    places = jnp.arange(number_of)

    def named(lengths, offset_by):
        used = int((lengths > 0).sum())
        fixed = max(1, used // 4)
        shifted = fixed + (places - fixed + offset_by * (used - fixed)) % max(1, number_of - fixed)
        return jnp.zeros((number_of,), jnp.int32).at[ranking[jnp.where(places < fixed, places, shifted)]].set(jnp.asarray(lengths, jnp.int32))

    lengths = jnp.where(number % 4 == 0, named(heavy_load, number // 4), named(ordinary, number - number // 4 - 1))
    mixed = jax.random.permutation(jax.random.fold_in(own, 3), number_of)
    giver, taker = mixed[0:number_of // 2 * 2:2], mixed[1:number_of // 2 * 2:2]
    slack = jnp.minimum(lengths[giver] - 1, bound - lengths[taker]) // 2
    slack = jnp.where((giver == ranking[0]) | (taker == ranking[0]) | (lengths[taker] == 0), 0, jnp.maximum(slack, 0))
    shifted = jax.random.randint(jax.random.fold_in(own, 4), (number_of // 2,), 0, 1 << 20) % (slack + 1)
    lengths = lengths.at[giver].add(-shifted).at[taker].add(shifted)
    labels = jnp.searchsorted(jnp.cumsum(lengths), jnp.arange(rows * top), side="right").astype(jnp.int32)
    grid = labels.reshape(top, rows).T
    grid = grid[jax.random.permutation(jax.random.fold_in(own, 1), rows)]
    offset_by = jax.random.randint(jax.random.fold_in(own, 2), (rows, 1), 0, top)
    return jnp.take_along_axis(grid, (jnp.arange(top)[None, :] + offset_by) % top, axis=1)


def load_shares(amount, total, reach, slope, full):
    portions = [(1 << 20) // math.isqrt(standing ** slope) + 1 for standing in range(1, amount + 1)]
    largest = reach if full else min(reach, max(-(-total // amount), total * portions[0] // sum(portions)))
    least = 1 if total - largest >= amount - 1 else 0
    holding, rest = [largest] + [least] * (amount - 1), total - largest - least * (amount - 1)
    while rest > 0:
        movable = [i for i in range(1, amount) if holding[i] < largest] or [i for i in range(1, amount) if holding[i] < reach]
        mass, remaining = sum([portions[i] for i in movable]), rest
        for i in movable:
            extra = min(reach - holding[i], max(1, remaining * portions[i] // mass), rest)
            holding[i] = holding[i] + extra
            rest = rest - extra
    return np.array(holding)


def bell_draw(own_key, shape, scale, most, cuts=(), kind=jnp.bfloat16):
    factor_of = steps_of(own_key, shape, cuts, -0.22, 0.18) if cuts else 1.0
    array = jax.random.normal(own_key, shape, jnp.float32) * scale * factor_of
    return jnp.minimum(jnp.maximum(array, -most), most).astype(kind)


def setup_inputs(seed: int = 0) -> dict:
    seeds = jax.random.split(jax.random.key(seed), 4)
    partials = draw_partials(jax.random.fold_in(seeds[3], 71), 0)
    sketch = bell_draw(seeds[1], (N_FSDP, N_REP, SLOTS, BS, RANK), 0.5, 3.0, ((0, 8), (1, 4)))
    owner_table_keys = jax.random.split(jax.random.fold_in(seeds[2], 1), NB // BLK_REP)
    owner_table_turns = jax.random.permutation(jax.random.fold_in(seeds[2], 3), NB // BLK_REP)
    owner_table = jax.vmap(lambda own, number: assign_block(jax.random.fold_in(seeds[2], 2), own, number, BLK_REP, N_FSDP, 1, SLOTS, 2))(owner_table_keys, owner_table_turns).reshape((NB, 1))
    return {"partials": partials, "sketch": sketch, "owner_table": owner_table}


DECAY = 0.9
DAMPING = 64.0
FIRST_AXES = (((0,), (0,)), ((), ()))
LAST_AXES = (((1,), (1,)), ((), ()))

def inverse_root(matrix, epsilon):
    identity = jnp.eye(matrix.shape[0], dtype=jnp.float32)
    trace_sum = jnp.trace(matrix) + epsilon
    current = matrix / trace_sum
    inverse = identity
    for repeat in range(NS_ITERS):
        middle = 1.5 * identity - 0.5 * jnp.dot(inverse, current, precision=lax.Precision.HIGHEST)
        current = jnp.dot(current, middle, precision=lax.Precision.HIGHEST)
        inverse = jnp.dot(middle, inverse, precision=lax.Precision.HIGHEST)
    return inverse / jnp.sqrt(trace_sum)

def precondition(gradient, current_sketch):
    identity = jnp.eye(current_sketch.shape[1], dtype=jnp.float32)
    projected = lax.dot_general(gradient, current_sketch, FIRST_AXES, preferred_element_type=jnp.float32).astype(jnp.bfloat16)
    gram_matrix = lax.dot_general(current_sketch, current_sketch, FIRST_AXES, preferred_element_type=jnp.float32).astype(jnp.bfloat16)
    powered = DECAY * jnp.dot(current_sketch, gram_matrix, preferred_element_type=jnp.float32) + jnp.dot(gradient, projected, preferred_element_type=jnp.float32)
    inner_gram = lax.dot_general(powered, powered, FIRST_AXES, precision=lax.Precision.HIGHEST)
    basis_full = jnp.dot(powered, inverse_root(inner_gram, 1e-06), precision=lax.Precision.HIGHEST)
    basis_low = basis_full.astype(jnp.bfloat16)
    coefficients = lax.dot_general(gradient, basis_low, FIRST_AXES, preferred_element_type=jnp.float32).astype(jnp.bfloat16)
    alignment = lax.dot_general(current_sketch, basis_low, FIRST_AXES, preferred_element_type=jnp.float32)
    energy = DECAY * lax.dot_general(alignment, alignment, FIRST_AXES, precision=lax.Precision.HIGHEST) + lax.dot_general(coefficients, coefficients, FIRST_AXES, preferred_element_type=jnp.float32)
    root_inverse = inverse_root(energy + DAMPING * identity, 0.0)
    inner_part = jnp.dot(energy, root_inverse, precision=lax.Precision.HIGHEST)
    new_block = jnp.dot(basis_full, inner_part, precision=lax.Precision.HIGHEST).astype(jnp.bfloat16)
    mix_matrix = math.sqrt(DAMPING) * root_inverse - identity
    side_terms = lax.dot_general(coefficients.astype(jnp.float32), mix_matrix, LAST_AXES, precision=lax.Precision.HIGHEST).astype(jnp.bfloat16)
    update_block = (gradient.astype(jnp.float32) + lax.dot_general(basis_low, side_terms, LAST_AXES, preferred_element_type=jnp.float32)).astype(jnp.bfloat16)
    return (update_block, new_block)

def reference(partials, sketch, owner_table):
    owner_ids = owner_table[:, 0]
    block_ids = jnp.arange(NB, dtype=jnp.int32)

    def reduce_block(block):
        replicas = lax.dynamic_index_in_dim(partials, block, axis=1, keepdims=False)
        summed = lax.optimization_barrier(jnp.sum(replicas.astype(jnp.float32), axis=0)).astype(jnp.bfloat16)
        wide = summed.astype(jnp.float32)
        return (summed, jnp.sum(wide * wide))
    gradients, squares = lax.map(reduce_block, block_ids)
    sum_squares = jnp.sum(squares)
    clip_limit = 0.5 * math.sqrt(NB * BS * BS)
    clip_factor = jnp.minimum(1.0, clip_limit / jnp.sqrt(sum_squares + 1e-06))
    slice_ids = block_ids // BLK_REP
    same_owner = (owner_ids[:, None] == owner_ids[None, :]) & (slice_ids[:, None] == slice_ids[None, :]) & (block_ids[:, None] < block_ids[None, :])
    rank_in = lax.optimization_barrier(jnp.sum(same_owner.astype(jnp.int32), axis=0))

    def per_block(block):
        gradient = (clip_factor * gradients[block].astype(jnp.float32)).astype(jnp.bfloat16)
        current_sketch = sketch[owner_ids[block], slice_ids[block], rank_in[block]]
        return precondition(gradient, current_sketch)
    update, fresh_blocks = lax.map(per_block, block_ids)
    new_sketch = sketch.at[owner_ids, slice_ids, rank_in].set(fresh_blocks)
    return (update, new_sketch)
```

```python
import functools
import math

import jax
import jax.numpy as jnp
from jax import lax
from jax.experimental import pallas as pl
from jax.experimental.pallas import tpu as pltpu
from jax.sharding import PartitionSpec as P

NS_ITERS = 5


DECAY = 0.9
DAMPING = 64.0
FIRST_AXES = (((0,), (0,)), ((), ()))
LAST_AXES = (((1,), (1,)), ((), ()))


def inverse_root(matrix, epsilon):
    identity = jnp.eye(matrix.shape[0], dtype=jnp.float32)
    trace_sum = jnp.trace(matrix) + epsilon
    current = matrix / trace_sum
    inverse = identity
    for repeat in range(NS_ITERS):
        middle = 1.5 * identity - 0.5 * jnp.dot(inverse, current, precision=lax.Precision.HIGHEST)
        current = jnp.dot(current, middle, precision=lax.Precision.HIGHEST)
        inverse = jnp.dot(middle, inverse, precision=lax.Precision.HIGHEST)
    return inverse / jnp.sqrt(trace_sum)


def precondition(gradient, current_sketch):
    identity = jnp.eye(current_sketch.shape[1], dtype=jnp.float32)
    projected = lax.dot_general(
        gradient, current_sketch, FIRST_AXES, preferred_element_type=jnp.float32
    ).astype(jnp.bfloat16)
    gram_matrix = lax.dot_general(
        current_sketch, current_sketch, FIRST_AXES, preferred_element_type=jnp.float32
    ).astype(jnp.bfloat16)
    powered = DECAY * jnp.dot(
        current_sketch, gram_matrix, preferred_element_type=jnp.float32
    ) + jnp.dot(gradient, projected, preferred_element_type=jnp.float32)
    inner_gram = lax.dot_general(powered, powered, FIRST_AXES, precision=lax.Precision.HIGHEST)
    basis_full = jnp.dot(powered, inverse_root(inner_gram, 1e-06), precision=lax.Precision.HIGHEST)
    basis_low = basis_full.astype(jnp.bfloat16)
    coefficients = lax.dot_general(
        gradient, basis_low, FIRST_AXES, preferred_element_type=jnp.float32
    ).astype(jnp.bfloat16)
    alignment = lax.dot_general(
        current_sketch, basis_low, FIRST_AXES, preferred_element_type=jnp.float32
    )
    energy = DECAY * lax.dot_general(
        alignment, alignment, FIRST_AXES, precision=lax.Precision.HIGHEST
    ) + lax.dot_general(coefficients, coefficients, FIRST_AXES, preferred_element_type=jnp.float32)
    root_inverse = inverse_root(energy + DAMPING * identity, 0.0)
    inner_part = jnp.dot(energy, root_inverse, precision=lax.Precision.HIGHEST)
    new_block = jnp.dot(basis_full, inner_part, precision=lax.Precision.HIGHEST).astype(
        jnp.bfloat16
    )
    mix_matrix = math.sqrt(DAMPING) * root_inverse - identity
    side_terms = lax.dot_general(
        coefficients.astype(jnp.float32), mix_matrix, LAST_AXES, precision=lax.Precision.HIGHEST
    ).astype(jnp.bfloat16)
    update_block = (
        gradient.astype(jnp.float32)
        + lax.dot_general(basis_low, side_terms, LAST_AXES, preferred_element_type=jnp.float32)
    ).astype(jnp.bfloat16)
    return (update_block, new_block)


def squared_sum(values):
    wide = values.astype(jnp.float32)
    return jnp.sum(wide * wide)


def process_slot(slot_index, arrived, clip_factor, held_sketches, filled):
    block_width = arrived.shape[-1]
    gradient = (clip_factor * arrived.reshape(block_width, block_width).astype(jnp.float32)).astype(
        jnp.bfloat16
    )
    current_sketch = held_sketches[slot_index]
    active = slot_index < filled
    update_block, new_block = precondition(gradient, current_sketch)
    new_block = jnp.where(active, new_block, current_sketch)
    return (update_block, new_block)


def local(partials, sketch, owner_table):
    block_total = partials.shape[1]
    row_count = partials.shape[2]
    block_width = partials.shape[3]
    fsdp_count = lax.axis_size("fsdp")
    per_slice = block_total // lax.axis_size("rep")
    slot_count = sketch.shape[2]
    reduced = lax.psum_scatter(
        partials[0].astype(jnp.float32).astype(jnp.bfloat16), "rep", scatter_dimension=0, tiled=True
    )
    my_owners = lax.dynamic_slice_in_dim(
        owner_table[:, 0], lax.axis_index("rep") * per_slice, per_slice
    )
    positions = jnp.arange(per_slice, dtype=jnp.int32)
    same_owner = (my_owners[:, None] == my_owners[None, :]) & (
        positions[:, None] < positions[None, :]
    )
    rank_in = jnp.sum(same_owner.astype(jnp.int32), axis=0)
    target = rank_in * fsdp_count + my_owners
    selector = (
        target[None, :] == jnp.arange(slot_count * fsdp_count, dtype=jnp.int32)[:, None]
    ).astype(jnp.bfloat16)
    flattened = reduced.reshape(per_slice, row_count * block_width)
    outgoing = jnp.dot(selector, flattened, preferred_element_type=jnp.float32).astype(jnp.bfloat16)
    outgoing = outgoing.reshape(slot_count, fsdp_count, row_count, block_width)
    sum_squares = lax.psum(squared_sum(reduced), ("fsdp", "rep"))
    clip_limit = 0.5 * math.sqrt(block_total * block_width * block_width)
    clip_factor = jnp.minimum(1.0, clip_limit / jnp.sqrt(sum_squares + 1e-06))
    filled = jnp.sum((my_owners == lax.axis_index("fsdp")).astype(jnp.int32))
    held_sketches = sketch[0, 0]
    fresh_list = []
    incoming = lax.all_to_all(outgoing, "fsdp", split_axis=1, concat_axis=1, tiled=True)
    update_list = []
    for slot_index in range(slot_count):
        update_block, new_block = process_slot(
            slot_index, incoming[slot_index], clip_factor, held_sketches, filled
        )
        update_list.append(update_block)
        fresh_list.append(new_block)
    stacked = jnp.stack(update_list).reshape(slot_count, fsdp_count, row_count, block_width)
    returned = lax.all_to_all(stacked, "fsdp", split_axis=1, concat_axis=1, tiled=True)
    returned = returned.reshape(slot_count * fsdp_count, row_count * block_width)
    my_updates = lax.dot_general(
        selector, returned, FIRST_AXES, preferred_element_type=jnp.float32
    ).astype(jnp.bfloat16)
    my_updates = my_updates.reshape(per_slice, row_count, block_width)
    return (my_updates, jnp.stack(fresh_list)[None, None])

MESH = pl.DeviceIdType.MESH
BF = jnp.bfloat16
F32 = jnp.float32


def flip(value, mask, bits):
    result = 0
    for bit in range(bits):
        ours = (value // (1 << bit)) % 2
        theirs = (mask // (1 << bit)) % 2
        result = result + (ours + theirs - 2 * ours * theirs) * (1 << bit)
    return result


def greet(peers):
    barrier = pltpu.get_barrier_semaphore()
    for peer in peers:
        pl.semaphore_signal(barrier, inc=1, device_id=peer, device_id_type=MESH)
    pl.semaphore_wait(barrier, len(peers))


def remote(source, target, send_sem, recv_sem, peer):
    return pltpu.make_async_remote_copy(
        src_ref=source,
        dst_ref=target,
        send_sem=send_sem,
        recv_sem=recv_sem,
        device_id=peer,
        device_id_type=MESH,
    )


def forward_kernel(
    fsdp, slots, index_ref, valid_ref, partials_ref, incoming_ref, squares_ref,
    held, staged, paired, far, crossed, summed, square_acc, rep_squares, fsdp_squares,
    load_sem, pair_sems, cross_sems, owner_sems, self_sem, rep_sems, fsdp_sems,
):
    bits = fsdp.bit_length() - 1
    half = fsdp // 2
    steps = slots * fsdp
    me_f = lax.axis_index("fsdp")
    me_r = lax.axis_index("rep")
    core = me_r % 2
    row = me_r // 2
    partner = row * 2 + 1 - core
    across = (1 - row) * 2 + core
    partner_across = (1 - row) * 2 + 1 - core

    load = pltpu.make_async_copy(partials_ref.at[0], held, load_sem)
    load.start()
    greet(
        [{"rep": (me_r + d) % 4} for d in range(1, 4)]
        + [{"fsdp": (me_f + d) % fsdp} for d in range(1, fsdp)]
    )
    load.wait()

    def where(i):
        group = i // (slots * half)
        slot = (i % (slots * half)) // half
        mask = fsdp - 1 - half * group - i % half
        return slot, mask, flip(me_f, mask, bits)

    def pair_copy(i):
        return remote(
            staged.at[i], paired.at[i], pair_sems.at[0, i], pair_sems.at[1, i], {"rep": partner}
        )

    def cross_copy(i):
        return remote(
            far.at[i], crossed.at[i], cross_sems.at[0, i], cross_sems.at[1, i], {"rep": across}
        )

    def owner_copy(i):
        slot, mask, owner = where(i)
        return remote(
            summed.at[i],
            incoming_ref.at[slot, me_f],
            owner_sems.at[0, i],
            owner_sems.at[1, i],
            {"fsdp": owner},
        )

    def self_copy(i):
        slot, mask, owner = where(i)
        return pltpu.make_async_copy(
            summed.at[i], incoming_ref.at[slot, me_f], self_sem.at[slot]
        )

    def stage(i, carry):
        slot, mask, owner = where(i)
        place = slot * fsdp + owner
        staged[i, 0] = held[index_ref[partner_across, place]]
        staged[i, 1] = held[index_ref[partner, place]]
        pair_copy(i).start()
        return carry

    lax.fori_loop(0, steps, stage, 0)
    square_acc[...] = jnp.zeros_like(square_acc)

    def send_across(i):
        slot, mask, owner = where(i)
        place = slot * fsdp + owner
        pair_copy(i).wait_recv()
        mine = held[index_ref[across, place]].astype(F32)
        far[i] = (mine + paired[i, 0].astype(F32)).astype(BF)
        cross_copy(i).start()

    def send_owner(i):
        slot, mask, owner = where(i)
        place = slot * fsdp + owner
        cross_copy(i).wait_recv()
        mine = held[index_ref[me_r, place]].astype(F32)
        total = (mine + paired[i, 1].astype(F32) + crossed[i].astype(F32)).astype(BF)
        summed[i] = total

        @pl.when(mask == 0)
        def _():
            self_copy(i).start()

        @pl.when(mask != 0)
        def _():
            owner_copy(i).start()

        wide = total.astype(F32)
        folded = jnp.sum((wide * wide).reshape(wide.shape[0] // 8, 8, wide.shape[1]), axis=0)
        square_acc[...] += folded * valid_ref[me_r, place]

    lag = 2

    def both(i, carry):
        @pl.when(i < steps)
        def _():
            send_across(i)

        @pl.when(i >= lag)
        def _():
            send_owner(i - lag)

        return carry

    lax.fori_loop(0, steps + lag, both, 0)

    lanes = square_acc[:, 0:128]
    for part in range(1, square_acc.shape[1] // 128):
        lanes = lanes + square_acc[:, part * 128 : (part + 1) * 128]
    rep_squares[me_r] = lanes
    copies = [
        remote(
            rep_squares.at[me_r], rep_squares.at[me_r], rep_sems.at[0, d], rep_sems.at[1, d],
            {"rep": (me_r + d) % 4},
        )
        for d in range(1, 4)
    ]
    for copy in copies:
        copy.start()
    for copy in copies:
        copy.wait()
    lanes = rep_squares[0]
    for r in range(1, 4):
        lanes = lanes + rep_squares[r]
    fsdp_squares[me_f] = lanes
    copies = [
        remote(
            fsdp_squares.at[me_f], fsdp_squares.at[me_f], fsdp_sems.at[0, d], fsdp_sems.at[1, d],
            {"fsdp": (me_f + d) % fsdp},
        )
        for d in range(1, fsdp)
    ]
    for copy in copies:
        copy.start()
    for copy in copies:
        copy.wait()
    lanes = fsdp_squares[0]
    for f in range(1, fsdp):
        lanes = lanes + fsdp_squares[f]
    squares_ref[...] = lanes

    def finish(i, carry):
        slot, mask, owner = where(i)
        pair_copy(i).wait_send()
        cross_copy(i).wait_send()

        @pl.when(mask == 0)
        def _():
            self_copy(i).wait()

        @pl.when(mask != 0)
        def _():
            owner_copy(i).wait()

        return carry

    lax.fori_loop(0, steps, finish, 0)


def mm(a, b):
    return jnp.dot(a, b, preferred_element_type=F32)


def mm_last(a, b):
    return lax.dot_general(a, b, LAST_AXES, preferred_element_type=F32)


def split(values):
    high = values.astype(BF)
    return high, (values - high.astype(F32)).astype(BF)


def mm3(a, b):
    return mm(a[0], b[0]) + (mm(a[0], b[1]) + mm(a[1], b[0]))


def eye_of(size):
    return (
        lax.broadcasted_iota(jnp.int32, (size, size), 0)
        == lax.broadcasted_iota(jnp.int32, (size, size), 1)
    ).astype(F32)


def kernel_root(matrix, epsilon, identity):
    trace_sum = jnp.sum(matrix * identity, keepdims=True) + epsilon
    current = matrix / trace_sum
    middle = 1.5 * identity - 0.5 * current
    middle_s = split(middle)
    inverse_s = middle_s
    current_s = split(mm3(split(current), middle_s))
    for repeat in range(1, NS_ITERS):
        middle_s = split(1.5 * identity - 0.5 * mm3(inverse_s, current_s))
        if repeat < NS_ITERS - 1:
            current_s = split(mm3(current_s, middle_s))
        inverse = mm3(middle_s, inverse_s)
        inverse_s = split(inverse)
    return inverse / jnp.sqrt(trace_sum)


def owner_kernel(
    fsdp, slots, clip_limit, active_ref, squares_ref, incoming_ref, sketch_ref, returned_ref, fresh_ref,
    held, updates, narrow_t, side_t, wide, basis, basis_low, load_sem, send_sems, recv_sems, self_sem,
):
    bits = fsdp.bit_length() - 1
    me_f = lax.axis_index("fsdp")
    rows = held.shape[2]
    width = held.shape[3]
    rank = sketch_ref.shape[2]
    tile = rank
    loads = [
        pltpu.make_async_copy(incoming_ref.at[k], held.at[k], load_sem.at[k]) for k in range(slots)
    ]
    for copy in loads:
        copy.start()
    greet([{"fsdp": (me_f + d) % fsdp} for d in range(1, fsdp)])
    sum_squares = jnp.sum(squares_ref[...], keepdims=True)
    clip_factor = jnp.minimum(1.0, clip_limit / jnp.sqrt(sum_squares + 1e-06))
    identity = eye_of(rank)

    def home_copy(k, i):
        home = flip(me_f, fsdp - 1 - i, bits)
        return remote(
            updates.at[k, i], returned_ref.at[k, me_f], send_sems.at[k, i], recv_sems.at[k, i],
            {"fsdp": home},
        )

    def self_copy(k):
        return pltpu.make_async_copy(
            updates.at[k, fsdp - 1], returned_ref.at[k, me_f], self_sem.at[k]
        )

    for k in range(slots):
        loads[k].wait()
        for part in range(fsdp):
            held[k, part] = (clip_factor * held[k, part].astype(F32)).astype(BF)
        sketch = sketch_ref[k]
        sketch_t = sketch.T

        def wide_part(part):
            return held[k, :, :, part * tile : (part + 1) * tile].reshape(width, tile)

        for part in range(width // tile):
            narrow_t[:, part * tile : (part + 1) * tile] = mm(sketch_t, wide_part(part)).astype(BF)
        gram = mm(sketch_t, sketch).astype(BF)
        projected_t = narrow_t[...]
        for part in range(fsdp):
            span = slice(part * rows, (part + 1) * rows)
            wide[span] = DECAY * mm(sketch[span], gram) + mm_last(held[k, part], projected_t)
        powered_s = split(wide[...])
        powered_t = powered_s[0].T
        mixed = mm(powered_t, powered_s[1])
        inner = mm(powered_t, powered_s[0]) + (mixed + mixed.T)
        root = split(kernel_root(inner, 1e-06, identity))
        full = mm3(powered_s, root)
        basis[...] = full
        low = full.astype(BF)
        basis_low[...] = low
        low_t = low.T
        for part in range(width // tile):
            narrow_t[:, part * tile : (part + 1) * tile] = mm(low_t, wide_part(part)).astype(BF)
        coefficients_t = narrow_t[...]
        alignment = mm(sketch_t, low)
        align_s = split(alignment)
        align_t = (align_s[0].T, align_s[1].T)
        energy = DECAY * mm3(align_t, align_s) + mm_last(coefficients_t, coefficients_t)
        root_inverse = kernel_root(energy + DAMPING * identity, 0.0, identity)
        mix = split(math.sqrt(DAMPING) * root_inverse - identity)
        side_t[...] = (mm(mix[0], coefficients_t) + mm(mix[1], coefficients_t)).astype(BF)

        def send(i, carry):
            home = flip(me_f, fsdp - 1 - i, bits)
            start = pl.multiple_of(home * rows, rows)
            updates[k, i] = (
                held[k, home].astype(F32) + mm(basis_low[pl.ds(start, rows), :], side_t[...])
            ).astype(BF)

            @pl.when(i == fsdp - 1)
            def _():
                self_copy(k).start()

            @pl.when(i != fsdp - 1)
            def _():
                home_copy(k, i).start()

            return carry

        lax.fori_loop(0, fsdp, send, 0)
        inner_part = split(mm3(split(energy), split(root_inverse)))
        new_block = mm3(split(basis[...]), inner_part).astype(BF)
        fresh_ref[k] = jnp.where(active_ref[k] > 0, new_block, sketch)

    def finish(i, carry):
        for k in range(slots):
            home_copy(k, i).wait()
        return carry

    lax.fori_loop(0, fsdp - 1, finish, 0)
    for k in range(slots):
        self_copy(k).wait()


def place_kernel(target_ref, returned_ref, update_ref):
    update_ref[...] = returned_ref[...]


def fused(partials, sketch, owner_table):
    block_total, rows, width = partials.shape[1:]
    rank = sketch.shape[4]
    fsdp = lax.axis_size("fsdp")
    rep = lax.axis_size("rep")
    slots = sketch.shape[2]
    per_slice = block_total // rep
    steps = slots * fsdp
    owners = owner_table[:, 0].reshape(rep, per_slice)
    positions = jnp.arange(per_slice, dtype=jnp.int32)
    same = (owners[:, :, None] == owners[:, None, :]) & (positions[:, None] < positions[None, :])
    target = jnp.sum(same.astype(jnp.int32), axis=1) * fsdp + owners
    hit = target[:, None, :] == jnp.arange(steps, dtype=jnp.int32)[:, None]
    numbers = jnp.arange(block_total, dtype=jnp.int32).reshape(rep, 1, per_slice)
    index = jnp.sum(jnp.where(hit, numbers, 0), axis=2)
    valid = jnp.sum(hit.astype(F32), axis=2)
    me_r = lax.axis_index("rep")
    my_target = lax.dynamic_index_in_dim(target, me_r, 0, keepdims=False)
    active = lax.dynamic_slice(
        lax.dynamic_index_in_dim(valid, me_r, 0, keepdims=False).reshape(slots, fsdp),
        (0, lax.axis_index("fsdp")), (slots, 1),
    )[:, 0]

    hbm = pl.BlockSpec(memory_space=pl.ANY)
    vmem = pl.BlockSpec(memory_space=pltpu.VMEM)
    smem = pl.BlockSpec(memory_space=pltpu.SMEM)
    dma = pltpu.SemaphoreType.DMA
    block = (rows, width)
    incoming, squares = pl.pallas_call(
        functools.partial(forward_kernel, fsdp, slots),
        out_shape=(
            jax.ShapeDtypeStruct((slots, fsdp) + block, BF),
            jax.ShapeDtypeStruct((8, 128), F32),
        ),
        in_specs=[smem, smem, hbm],
        out_specs=(hbm, vmem),
        scratch_shapes=[
            pltpu.VMEM((block_total,) + block, BF),
            pltpu.VMEM((steps, 2) + block, BF),
            pltpu.VMEM((steps, 2) + block, BF),
            pltpu.VMEM((steps,) + block, BF),
            pltpu.VMEM((steps,) + block, BF),
            pltpu.VMEM((steps,) + block, BF),
            pltpu.VMEM((8, width), F32),
            pltpu.VMEM((rep, 8, 128), F32),
            pltpu.VMEM((fsdp, 8, 128), F32),
            dma,
            dma((2, steps)),
            dma((2, steps)),
            dma((2, steps)),
            dma((slots,)),
            dma((2, rep)),
            dma((2, fsdp)),
        ],
        compiler_params=pltpu.CompilerParams(
            collective_id=0, has_side_effects=True, vmem_limit_bytes=VMEM_BYTES
        ),
        name="forward",
    )(index, valid, partials)
    clip_limit = 0.5 * math.sqrt(block_total * width * width)
    returned, fresh = pl.pallas_call(
        functools.partial(owner_kernel, fsdp, slots, clip_limit),
        out_shape=(
            jax.ShapeDtypeStruct((slots, fsdp) + block, BF),
            jax.ShapeDtypeStruct((slots, width, rank), BF),
        ),
        in_specs=[smem, vmem, hbm, vmem],
        out_specs=(hbm, vmem),
        scratch_shapes=[
            pltpu.VMEM((slots, fsdp) + block, BF),
            pltpu.VMEM((slots, fsdp) + block, BF),
            pltpu.VMEM((rank, width), BF),
            pltpu.VMEM((rank, width), BF),
            pltpu.VMEM((width, rank), F32),
            pltpu.VMEM((width, rank), F32),
            pltpu.VMEM((width, rank), BF),
            dma((slots,)),
            dma((slots, fsdp)),
            dma((slots, fsdp)),
            dma((slots,)),
        ],
        compiler_params=pltpu.CompilerParams(
            collective_id=1, has_side_effects=True, vmem_limit_bytes=VMEM_BYTES
        ),
        name="owner",
    )(active, squares, incoming, sketch[0, 0])
    returned = returned.reshape((steps,) + block)
    updates = pl.pallas_call(
        place_kernel,
        out_shape=jax.ShapeDtypeStruct((per_slice,) + block, BF),
        grid_spec=pltpu.PrefetchScalarGridSpec(
            num_scalar_prefetch=1,
            grid=(per_slice,),
            in_specs=[pl.BlockSpec((1,) + block, lambda b, t: (t[b], 0, 0))],
            out_specs=pl.BlockSpec((1,) + block, lambda b, t: (b, 0, 0)),
        ),
        name="place",
    )(my_target, returned)
    return (updates, fresh[None, None])


VMEM_BYTES = 60 * 1024 * 1024


def choose(partials, sketch, owner_table):
    block_total, rows, width = partials.shape[1:]
    fsdp = lax.axis_size("fsdp")
    rep = lax.axis_size("rep")
    steps = sketch.shape[2] * fsdp
    pairs = rep == 4 and fsdp & (fsdp - 1) == 0
    needed = (block_total + 7 * steps) * rows * width * 2
    if pairs and needed < VMEM_BYTES - (1 << 21):
        return fused(partials, sketch, owner_table)
    return local(partials, sketch, owner_table)


def solution(mesh):
    placed = (P("rep", None, "fsdp", None), P("fsdp", "rep", None, None, None), P())
    return jax.shard_map(
        choose,
        mesh=mesh,
        in_specs=placed,
        out_specs=(P("rep", "fsdp", None), P("fsdp", "rep", None, None, None)),
        check_vma=False,
    )
```

```python
import functools
import math

import jax
import jax.numpy as jnp
from jax import lax
from jax.experimental import pallas as pl
from jax.experimental.pallas import tpu as pltpu
from jax.sharding import PartitionSpec as P

NS_ITERS = 5


DECAY = 0.9
DAMPING = 64.0
FIRST_AXES = (((0,), (0,)), ((), ()))
LAST_AXES = (((1,), (1,)), ((), ()))


def inverse_root(matrix, epsilon):
    identity = jnp.eye(matrix.shape[0], dtype=jnp.float32)
    trace_sum = jnp.trace(matrix) + epsilon
    current = matrix / trace_sum
    inverse = identity
    for repeat in range(NS_ITERS):
        middle = 1.5 * identity - 0.5 * jnp.dot(inverse, current, precision=lax.Precision.HIGHEST)
        current = jnp.dot(current, middle, precision=lax.Precision.HIGHEST)
        inverse = jnp.dot(middle, inverse, precision=lax.Precision.HIGHEST)
    return inverse / jnp.sqrt(trace_sum)


def precondition(gradient, current_sketch):
    identity = jnp.eye(current_sketch.shape[1], dtype=jnp.float32)
    projected = lax.dot_general(
        gradient, current_sketch, FIRST_AXES, preferred_element_type=jnp.float32
    ).astype(jnp.bfloat16)
    gram_matrix = lax.dot_general(
        current_sketch, current_sketch, FIRST_AXES, preferred_element_type=jnp.float32
    ).astype(jnp.bfloat16)
    powered = DECAY * jnp.dot(
        current_sketch, gram_matrix, preferred_element_type=jnp.float32
    ) + jnp.dot(gradient, projected, preferred_element_type=jnp.float32)
    inner_gram = lax.dot_general(powered, powered, FIRST_AXES, precision=lax.Precision.HIGHEST)
    basis_full = jnp.dot(powered, inverse_root(inner_gram, 1e-06), precision=lax.Precision.HIGHEST)
    basis_low = basis_full.astype(jnp.bfloat16)
    coefficients = lax.dot_general(
        gradient, basis_low, FIRST_AXES, preferred_element_type=jnp.float32
    ).astype(jnp.bfloat16)
    alignment = lax.dot_general(
        current_sketch, basis_low, FIRST_AXES, preferred_element_type=jnp.float32
    )
    energy = DECAY * lax.dot_general(
        alignment, alignment, FIRST_AXES, precision=lax.Precision.HIGHEST
    ) + lax.dot_general(coefficients, coefficients, FIRST_AXES, preferred_element_type=jnp.float32)
    root_inverse = inverse_root(energy + DAMPING * identity, 0.0)
    inner_part = jnp.dot(energy, root_inverse, precision=lax.Precision.HIGHEST)
    new_block = jnp.dot(basis_full, inner_part, precision=lax.Precision.HIGHEST).astype(
        jnp.bfloat16
    )
    mix_matrix = math.sqrt(DAMPING) * root_inverse - identity
    side_terms = lax.dot_general(
        coefficients.astype(jnp.float32), mix_matrix, LAST_AXES, precision=lax.Precision.HIGHEST
    ).astype(jnp.bfloat16)
    update_block = (
        gradient.astype(jnp.float32)
        + lax.dot_general(basis_low, side_terms, LAST_AXES, preferred_element_type=jnp.float32)
    ).astype(jnp.bfloat16)
    return (update_block, new_block)


def squared_sum(values):
    wide = values.astype(jnp.float32)
    return jnp.sum(wide * wide)


def process_slot(slot_index, arrived, clip_factor, held_sketches, filled):
    block_width = arrived.shape[-1]
    gradient = (clip_factor * arrived.reshape(block_width, block_width).astype(jnp.float32)).astype(
        jnp.bfloat16
    )
    current_sketch = held_sketches[slot_index]
    active = slot_index < filled
    update_block, new_block = precondition(gradient, current_sketch)
    new_block = jnp.where(active, new_block, current_sketch)
    return (update_block, new_block)


def local(partials, sketch, owner_table):
    block_total = partials.shape[1]
    row_count = partials.shape[2]
    block_width = partials.shape[3]
    fsdp_count = lax.axis_size("fsdp")
    per_slice = block_total // lax.axis_size("rep")
    slot_count = sketch.shape[2]
    reduced = lax.psum_scatter(
        partials[0].astype(jnp.float32).astype(jnp.bfloat16), "rep", scatter_dimension=0, tiled=True
    )
    my_owners = lax.dynamic_slice_in_dim(
        owner_table[:, 0], lax.axis_index("rep") * per_slice, per_slice
    )
    positions = jnp.arange(per_slice, dtype=jnp.int32)
    same_owner = (my_owners[:, None] == my_owners[None, :]) & (
        positions[:, None] < positions[None, :]
    )
    rank_in = jnp.sum(same_owner.astype(jnp.int32), axis=0)
    target = rank_in * fsdp_count + my_owners
    selector = (
        target[None, :] == jnp.arange(slot_count * fsdp_count, dtype=jnp.int32)[:, None]
    ).astype(jnp.bfloat16)
    flattened = reduced.reshape(per_slice, row_count * block_width)
    outgoing = jnp.dot(selector, flattened, preferred_element_type=jnp.float32).astype(jnp.bfloat16)
    outgoing = outgoing.reshape(slot_count, fsdp_count, row_count, block_width)
    sum_squares = lax.psum(squared_sum(reduced), ("fsdp", "rep"))
    clip_limit = 0.5 * math.sqrt(block_total * block_width * block_width)
    clip_factor = jnp.minimum(1.0, clip_limit / jnp.sqrt(sum_squares + 1e-06))
    filled = jnp.sum((my_owners == lax.axis_index("fsdp")).astype(jnp.int32))
    held_sketches = sketch[0, 0]
    fresh_list = []
    incoming = lax.all_to_all(outgoing, "fsdp", split_axis=1, concat_axis=1, tiled=True)
    update_list = []
    for slot_index in range(slot_count):
        update_block, new_block = process_slot(
            slot_index, incoming[slot_index], clip_factor, held_sketches, filled
        )
        update_list.append(update_block)
        fresh_list.append(new_block)
    stacked = jnp.stack(update_list).reshape(slot_count, fsdp_count, row_count, block_width)
    returned = lax.all_to_all(stacked, "fsdp", split_axis=1, concat_axis=1, tiled=True)
    returned = returned.reshape(slot_count * fsdp_count, row_count * block_width)
    my_updates = lax.dot_general(
        selector, returned, FIRST_AXES, preferred_element_type=jnp.float32
    ).astype(jnp.bfloat16)
    my_updates = my_updates.reshape(per_slice, row_count, block_width)
    return (my_updates, jnp.stack(fresh_list)[None, None])

MESH = pl.DeviceIdType.MESH
BF = jnp.bfloat16
F32 = jnp.float32


def flip(value, mask, bits):
    result = 0
    for bit in range(bits):
        ours = (value // (1 << bit)) % 2
        theirs = (mask // (1 << bit)) % 2
        result = result + (ours + theirs - 2 * ours * theirs) * (1 << bit)
    return result


def greet(peers):
    barrier = pltpu.get_barrier_semaphore()
    for peer in peers:
        pl.semaphore_signal(barrier, inc=1, device_id=peer, device_id_type=MESH)
    pl.semaphore_wait(barrier, len(peers))


def remote(source, target, send_sem, recv_sem, peer):
    return pltpu.make_async_remote_copy(
        src_ref=source,
        dst_ref=target,
        send_sem=send_sem,
        recv_sem=recv_sem,
        device_id=peer,
        device_id_type=MESH,
    )


def mm(a, b):
    return jnp.dot(a, b, preferred_element_type=F32)


def mm_last(a, b):
    return lax.dot_general(a, b, LAST_AXES, preferred_element_type=F32)


def split(values):
    high = values.astype(BF)
    return high, (values - high.astype(F32)).astype(BF)


def mm3(a, b):
    return mm(a[0], b[0]) + (mm(a[0], b[1]) + mm(a[1], b[0]))


def eye_of(size):
    return (
        lax.broadcasted_iota(jnp.int32, (size, size), 0)
        == lax.broadcasted_iota(jnp.int32, (size, size), 1)
    ).astype(F32)


def kernel_root(matrix, epsilon, identity):
    trace_sum = jnp.sum(matrix * identity, keepdims=True) + epsilon
    current = matrix / trace_sum
    middle = 1.5 * identity - 0.5 * current
    middle_s = split(middle)
    inverse_s = middle_s
    current_s = split(mm3(split(current), middle_s))
    for repeat in range(1, NS_ITERS):
        middle_s = split(1.5 * identity - 0.5 * mm3(inverse_s, current_s))
        if repeat < NS_ITERS - 1:
            current_s = split(mm3(current_s, middle_s))
        inverse = mm3(middle_s, inverse_s)
        inverse_s = split(inverse)
    return inverse / jnp.sqrt(trace_sum)


def step_kernel(
    fsdp, slots, per_slice, clip_limit, owners_ref, sketch_ref, partials_ref, returned_ref, fresh_ref,
    held_far, held_own, paired_far, paired_own, far, crossed, summed, incoming, updates, narrow_t, side_t, wide, basis, basis_low,
    square_acc, rep_squares, fsdp_squares, table, scalars,
    load_sems, pair_sems, cross_sems, owner_sems, rep_sems, fsdp_sems, home_sems, self_sems, table_sem,
):
    bits = fsdp.bit_length() - 1
    half = fsdp // 2
    steps = slots * fsdp
    rows = incoming.shape[2]
    width = incoming.shape[3]
    rank = sketch_ref.shape[2]
    tile = rank
    me_f = lax.axis_index("fsdp")
    me_r = lax.axis_index("rep")
    core = me_r % 2
    row = me_r // 2
    partner = row * 2 + 1 - core
    across = (1 - row) * 2 + core
    partner_across = (1 - row) * 2 + 1 - core

    def blocks_of(number):
        return partials_ref.at[0, pl.ds(number * per_slice, per_slice)]

    loads = [
        pltpu.make_async_copy(blocks_of(across), held_far, load_sems.at[0]),
        pltpu.make_async_copy(blocks_of(me_r), held_own, load_sems.at[1]),
    ]
    pairs = [
        remote(
            blocks_of(theirs), landing, pair_sems.at[0, n], pair_sems.at[1, n], {"rep": partner}
        )
        for n, (theirs, landing) in enumerate(
            ((partner_across, paired_far), (partner, paired_own))
        )
    ]
    loads[0].start()
    fill_table(fsdp, slots, per_slice, owners_ref, table)
    greet(
        [{"rep": (me_r + d) % 4} for d in range(1, 4)]
        + [{"fsdp": (me_f + d) % fsdp} for d in range(1, fsdp)]
    )
    pairs[0].start()
    pairs[1].start()
    loads[1].start()
    publish = pltpu.make_async_copy(table, scalars, table_sem)
    publish.start()
    square_acc[...] = jnp.zeros_like(square_acc)
    publish.wait()
    loads[0].wait()
    pairs[0].wait_recv()

    def where(i):
        group = i // (slots * half)
        slot = (i % (slots * half)) // half
        mask = fsdp - 1 - half * group - i % half
        return slot, mask, flip(me_f, mask, bits)

    def cross_copy(i):
        return remote(
            far.at[i], crossed.at[i], cross_sems.at[0, i], cross_sems.at[1, i], {"rep": across}
        )

    def owner_copy(i):
        slot, mask, owner = where(i)
        return remote(
            summed.at[i],
            incoming.at[slot, me_f],
            owner_sems.at[0, i],
            owner_sems.at[1, i],
            {"fsdp": owner},
        )

    def send_across(i):
        slot, mask, owner = where(i)
        number = scalars[0, across * steps + slot * fsdp + owner]
        far[i] = (held_far[number].astype(F32) + paired_far[number].astype(F32)).astype(BF)
        cross_copy(i).start()

    def send_owner(i):
        slot, mask, owner = where(i)
        place = me_r * steps + slot * fsdp + owner
        number = scalars[0, place]
        cross_copy(i).wait_recv()
        pair = held_own[number].astype(F32) + paired_own[number].astype(F32)
        total = (pair + crossed[i].astype(F32)).astype(BF)

        @pl.when(mask == 0)
        def _():
            incoming[slot, me_f] = total

        @pl.when(mask != 0)
        def _():
            summed[i] = total
            owner_copy(i).start()

        wide_total = total.astype(F32)
        folded = jnp.sum((wide_total * wide_total).reshape(rows // 8, 8, width), axis=0)
        square_acc[...] += jnp.where(scalars[1, place] > 0, folded, 0.0)

    lag = 2

    def first(i, carry):
        send_across(i)
        return carry

    lax.fori_loop(0, lag, first, 0)
    loads[1].wait()
    pairs[1].wait_recv()

    def both(i, carry):
        @pl.when(i < steps - lag)
        def _():
            send_across(i + lag)

        send_owner(i)
        return carry

    lax.fori_loop(0, steps, both, 0)

    def arrived(k):
        def wait_one(n, carry):
            i = (n // half) * (slots * half) + k * half + n % half
            owner_copy(i).wait_recv()
            return carry

        lax.fori_loop(0, fsdp - 1, wait_one, 0)

    def wide_part(k, part):
        return incoming[k, :, :, part * tile : (part + 1) * tile].reshape(width, tile)

    def project(k, left_t, factor):
        for part in range(width // tile):
            product = mm(left_t, wide_part(k, part))
            if factor is not None:
                product = factor * product
            narrow_t[:, part * tile : (part + 1) * tile] = product.astype(BF)

    lanes = square_acc[:, 0:128]
    for part in range(1, width // 128):
        lanes = lanes + square_acc[:, part * 128 : (part + 1) * 128]
    rep_squares[me_r] = lanes
    rep_copies = [
        remote(
            rep_squares.at[me_r], rep_squares.at[me_r], rep_sems.at[0, d], rep_sems.at[1, d],
            {"rep": (me_r + d) % 4},
        )
        for d in range(1, 4)
    ]
    for copy in rep_copies:
        copy.start()
    arrived(0)
    sketch_t = sketch_ref[0].T
    project(0, sketch_t, None)
    for copy in rep_copies:
        copy.wait()
    lanes = rep_squares[0]
    for r in range(1, 4):
        lanes = lanes + rep_squares[r]
    fsdp_squares[me_f] = lanes
    fsdp_copies = [
        remote(
            fsdp_squares.at[me_f], fsdp_squares.at[me_f], fsdp_sems.at[0, d], fsdp_sems.at[1, d],
            {"fsdp": (me_f + d) % fsdp},
        )
        for d in range(1, fsdp)
    ]
    for copy in fsdp_copies:
        copy.start()
    identity = eye_of(rank)

    def home_copy(k, i):
        home = flip(me_f, fsdp - 1 - i, bits)
        return remote(
            updates.at[k, i], returned_ref.at[k, me_f], home_sems.at[0, k, i], home_sems.at[1, k, i],
            {"fsdp": home},
        )

    def self_copy(k):
        return pltpu.make_async_copy(
            updates.at[k, fsdp - 1], returned_ref.at[k, me_f], self_sems.at[k]
        )

    clip_factor = None
    for k in range(slots):
        sketch = sketch_ref[k]
        if k > 0:
            arrived(k)
            sketch_t = sketch.T
            project(k, sketch_t, None)
        gram = mm(sketch_t, sketch).astype(BF)
        projected_t = narrow_t[...]
        for part in range(fsdp):
            span = slice(part * rows, (part + 1) * rows)
            wide[span] = mm_last(incoming[k, part], projected_t)
            basis[span] = DECAY * mm(sketch[span], gram)
        if k == 0:
            for copy in fsdp_copies:
                copy.wait()
            lanes = fsdp_squares[0]
            for f in range(1, fsdp):
                lanes = lanes + fsdp_squares[f]
            sum_squares = jnp.sum(lanes, keepdims=True)
            clip_factor = jnp.minimum(1.0, clip_limit / jnp.sqrt(sum_squares + 1e-06))
        powered_s = split(basis[...] + (clip_factor * clip_factor) * wide[...])
        powered_t = powered_s[0].T
        mixed = mm(powered_t, powered_s[1])
        inner = mm(powered_t, powered_s[0]) + (mixed + mixed.T)
        root = split(kernel_root(inner, 1e-06, identity))
        full = mm3(powered_s, root)
        basis[...] = full
        low = full.astype(BF)
        basis_low[...] = low
        project(k, low.T, clip_factor)
        coefficients_t = narrow_t[...]
        align_s = split(mm(sketch_t, low))
        align_t = (align_s[0].T, align_s[1].T)
        energy = DECAY * mm3(align_t, align_s) + mm_last(coefficients_t, coefficients_t)
        root_inverse = kernel_root(energy + DAMPING * identity, 0.0, identity)
        mix = split(math.sqrt(DAMPING) * root_inverse - identity)
        side_t[...] = (mm(mix[0], coefficients_t) + mm(mix[1], coefficients_t)).astype(BF)

        def send(i, carry):
            home = flip(me_f, fsdp - 1 - i, bits)
            start = pl.multiple_of(home * rows, rows)
            gradient = (clip_factor * incoming[k, home].astype(F32)).astype(BF).astype(F32)
            updates[k, i] = (
                gradient + mm(basis_low[pl.ds(start, rows), :], side_t[...])
            ).astype(BF)

            @pl.when(i == fsdp - 1)
            def _():
                self_copy(k).start()

            @pl.when(i != fsdp - 1)
            def _():
                home_copy(k, i).start()

            return carry

        lax.fori_loop(0, fsdp, send, 0)
        inner_part = split(mm3(split(energy), split(root_inverse)))
        new_block = mm3(split(basis[...]), inner_part).astype(BF)
        active = scalars[1, me_r * steps + k * fsdp + me_f]
        fresh_ref[k] = jnp.where(active > 0, new_block, sketch)

    pairs[0].wait_send()
    pairs[1].wait_send()

    def finish(i, carry):
        slot, mask, owner = where(i)
        cross_copy(i).wait_send()

        @pl.when(mask != 0)
        def _():
            owner_copy(i).wait_send()

        return carry

    lax.fori_loop(0, steps, finish, 0)

    def finish_home(i, carry):
        for k in range(slots):
            home_copy(k, i).wait()
        return carry

    lax.fori_loop(0, fsdp - 1, finish_home, 0)
    for k in range(slots):
        self_copy(k).wait()


def fill_table(fsdp, slots, per_slice, owners_ref, table):
    total = owners_ref.shape[0]
    steps = slots * fsdp
    shape = (total, total)
    down = lax.broadcasted_iota(jnp.int32, shape, 0)
    along = lax.broadcasted_iota(jnp.int32, shape, 1)
    owners = jnp.broadcast_to(owners_ref[...], shape)
    owners_along = jnp.sum(jnp.where(down == along, owners, 0), axis=0, keepdims=True)
    slice_down = down // per_slice
    slice_along = along // per_slice
    same = (owners == owners_along) & (slice_down == slice_along) & (along < down)
    ranks = jnp.sum(jnp.where(same, 1, 0), axis=1, keepdims=True)
    shape = (total, table.shape[1])
    block = lax.broadcasted_iota(jnp.int32, shape, 0)
    owned = jnp.broadcast_to(owners_ref[...], shape)
    target = (block // per_slice) * steps + jnp.broadcast_to(ranks, shape) * fsdp + owned
    hit = target == lax.broadcasted_iota(jnp.int32, shape, 1)
    number = jnp.sum(jnp.where(hit, block % per_slice, 0), axis=0, keepdims=True)
    table[0:1, :] = jnp.minimum(number, per_slice - 1)
    table[1:2, :] = jnp.sum(jnp.where(hit, 1, 0), axis=0, keepdims=True)


def place_kernel(fsdp, per_slice, owners_ref, returned_ref, update_ref, held, counts, in_sems, out_sems):
    base = lax.axis_index("rep") * per_slice
    last = returned_ref.shape[0] - 1
    for owner in range(fsdp):
        counts[owner] = 0
    takes, puts = [], []
    for b in range(per_slice):
        owner = owners_ref[base + b, 0]
        count = counts[owner]
        counts[owner] = count + 1
        takes.append(
            pltpu.make_async_copy(returned_ref.at[jnp.minimum(count, last), owner], held.at[b], in_sems.at[b])
        )
        takes[-1].start()
    for b in range(per_slice):
        takes[b].wait()
        puts.append(pltpu.make_async_copy(held.at[b], update_ref.at[b], out_sems.at[b]))
        puts[-1].start()
    for put in puts:
        put.wait()


def fused(partials, sketch, owner_table):
    block_total, rows, width = partials.shape[1:]
    rank = sketch.shape[4]
    fsdp = lax.axis_size("fsdp")
    rep = lax.axis_size("rep")
    slots = sketch.shape[2]
    per_slice = block_total // rep
    steps = slots * fsdp
    table_width = -(-rep * steps // 128) * 128
    hbm = pl.BlockSpec(memory_space=pl.ANY)
    vmem = pl.BlockSpec(memory_space=pltpu.VMEM)
    smem = pl.BlockSpec(memory_space=pltpu.SMEM)
    dma = pltpu.SemaphoreType.DMA
    block = (rows, width)
    clip_limit = 0.5 * math.sqrt(block_total * width * width)
    returned, fresh = pl.pallas_call(
        functools.partial(step_kernel, fsdp, slots, per_slice, clip_limit),
        out_shape=(
            jax.ShapeDtypeStruct((slots, fsdp) + block, BF),
            jax.ShapeDtypeStruct((slots, width, rank), BF),
        ),
        in_specs=[vmem, vmem, hbm],
        out_specs=(hbm, vmem),
        scratch_shapes=[
            pltpu.VMEM((per_slice,) + block, BF),
            pltpu.VMEM((per_slice,) + block, BF),
            pltpu.VMEM((per_slice,) + block, BF),
            pltpu.VMEM((per_slice,) + block, BF),
            pltpu.VMEM((steps,) + block, BF),
            pltpu.VMEM((steps,) + block, BF),
            pltpu.VMEM((steps,) + block, BF),
            pltpu.VMEM((slots, fsdp) + block, BF),
            pltpu.VMEM((slots, fsdp) + block, BF),
            pltpu.VMEM((rank, width), BF),
            pltpu.VMEM((rank, width), BF),
            pltpu.VMEM((width, rank), F32),
            pltpu.VMEM((width, rank), F32),
            pltpu.VMEM((width, rank), BF),
            pltpu.VMEM((8, width), F32),
            pltpu.VMEM((rep, 8, 128), F32),
            pltpu.VMEM((fsdp, 8, 128), F32),
            pltpu.VMEM((2, table_width), jnp.int32),
            pltpu.SMEM((2, table_width), jnp.int32),
            dma((2,)),
            dma((2, 2)),
            dma((2, steps)),
            dma((2, steps)),
            dma((2, rep)),
            dma((2, fsdp)),
            dma((2, slots, fsdp)),
            dma((slots,)),
            dma,
        ],
        compiler_params=pltpu.CompilerParams(
            collective_id=0, has_side_effects=True, vmem_limit_bytes=VMEM_BYTES
        ),
        name="step",
    )(owner_table, sketch[0, 0], partials)
    updates = pl.pallas_call(
        functools.partial(place_kernel, fsdp, per_slice),
        out_shape=jax.ShapeDtypeStruct((per_slice,) + block, BF),
        in_specs=[smem, hbm],
        out_specs=hbm,
        scratch_shapes=[
            pltpu.VMEM((per_slice,) + block, BF),
            pltpu.SMEM((fsdp,), jnp.int32),
            dma((per_slice,)),
            dma((per_slice,)),
        ],
        name="place",
    )(owner_table, returned)
    return (updates, fresh[None, None])


VMEM_BYTES = 60 * 1024 * 1024


def choose(partials, sketch, owner_table):
    block_total, rows, width = partials.shape[1:]
    fsdp = lax.axis_size("fsdp")
    rep = lax.axis_size("rep")
    steps = sketch.shape[2] * fsdp
    per_slice = block_total // rep
    pairs = rep == 4 and fsdp & (fsdp - 1) == 0
    needed = (4 * per_slice + 5 * steps) * rows * width * 2
    if pairs and needed < VMEM_BYTES - (12 << 20):
        return fused(partials, sketch, owner_table)
    return local(partials, sketch, owner_table)


def solution(mesh):
    placed = (P("rep", None, "fsdp", None), P("fsdp", "rep", None, None, None), P())
    return jax.shard_map(
        choose,
        mesh=mesh,
        in_specs=placed,
        out_specs=(P("rep", "fsdp", None), P("fsdp", "rep", None, None, None)),
        check_vma=False,
    )
```
